512 devices in a mesh: dp: 2 (over y_lo), ctx: 16 (over y_hi, x, core), tensor: 16 (over z).
Axes of the slice: x: 4, y: 4 (y_hi: 2, y_lo: 2; y = y_hi * 2 + y_lo), z: 16, core: 2. Of those that a mesh axis runs over, the one named last changes fastest.
Arguments:
- residual: bfloat16 [8192, 3584], P(('dp', 'ctx', 'tensor')), parts along dimension 0, may hold values from -6 to 6
- queries: bfloat16 [8192, 4096], P(('dp', 'ctx'), 'tensor'), parts along dimension 0, may hold values from -8 to 8
- key_heads: bfloat16 [8192, 2048], P(('dp', 'ctx'), 'tensor'), parts along dimension 0, may hold values from -8 to 8
- value_heads: bfloat16 [8192, 2048], P(('dp', 'ctx'), 'tensor'), parts along dimension 0, may hold values from -6 to 6
- doc_blocks: int32 [12], P('dp'), parts along dimension 0, may hold values from 1 to 64, 128 in all
- out_weight: bfloat16 [4096, 3584], P('tensor'), may hold values from -0.265625 to 0.265625
- post_gain: float32 [3584], replicated, may hold values from 0.1 to 1.9
- ffn_gain: float32 [3584], replicated, may hold values from 0.1 to 1.9
- gate_weight: bfloat16 [3584, 14336], P('ctx', 'tensor'), may hold values from -0.09375 to 0.09375
- up_weight: bfloat16 [3584, 14336], P('ctx', 'tensor'), may hold values from -0.09375 to 0.09375
Outputs:
- mixed_stream: bfloat16 [8192, 3584], P(('dp', 'ctx', 'tensor')), parts along dimension 0
- ffn_hidden: bfloat16 [8192, 14336], P(('dp', 'ctx'), 'tensor'), parts along dimension 0
The draws below stay inside these ranges and needn't reach their ends.
There are 2 independent parts, one for each index of `dp`. The reference program is written for one: setup_inputs(seed, part) draws one part's arguments, and reference() takes and returns one part's arrays. A program takes and returns all parts, laid end to end along the dimension named above; an argument that names none is the same for every part. Nothing has to cross between parts.
Inputs may be any that keep to these rules, and one draw needn't show every extreme that they name: `doc_blocks`: the lengths, in blocks of 32 positions, of the 6 documents packed in order into the sequence; they sum to 128, and the longest has exactly 64 blocks.
All inputs are finite; a program needn't handle non-finite values.
Results may differ from the reference program's by a relative error of at most 0.025.
Values may be sent and summed in bfloat16 or wider, within the bound.
A program may use at most 64 MiB of HBM per device.

```python
import math
import jax
import jax.numpy as jnp
import numpy as np
from jax import lax

D = 3584
HD = 256
H = 16
KVH = 8
FF = 14336
TOK_CTX = 256
LENGTH = 4096
BLOCK = 32
NBLK = 128
DOCS = 6
MOST_BLK = 64


def draw_out_weight(key, part):
    fan_rows = H * HD
    drawn = jnp.clip(jax.random.normal(key, (fan_rows, D), jnp.float32), -5.0, 5.0) * fan_rows ** (-0.5)
    return drawn.astype(jnp.bfloat16)


def background(key, array_shape):
    sample = jnp.clip(jax.random.normal(key, array_shape, jnp.float32), -6.0, 6.0)
    return sample


def aligned_plan(key):
    plan_key = jax.random.fold_in(key, 7301)
    block_shape = (NBLK, 1, KVH)
    marked = jax.random.randint(jax.random.fold_in(plan_key, 1), block_shape, 0, 2) == 0
    offset = jax.random.randint(jax.random.fold_in(plan_key, 2), block_shape, 0, BLOCK // 2)
    which_query = jax.random.randint(jax.random.fold_in(plan_key, 3), block_shape, 0, 2)
    own_higher = jax.random.randint(jax.random.fold_in(plan_key, 4), block_shape, 0, 2) == 1
    sign_table = (jax.random.randint(jax.random.fold_in(plan_key, 5), (NBLK, 1, KVH, HD), 0, 2) * 2 - 1).astype(jnp.float32)
    places = jnp.arange(BLOCK, dtype=jnp.int32)[None, :, None]
    own_hit = marked & (places == 2 * offset + 1)
    prev_hit = marked & (places == 2 * offset)
    dim_index = jnp.arange(HD, dtype=jnp.int32)
    slow_dims = (dim_index % (HD // 2) >= HD // 4).astype(jnp.float32)
    pattern = sign_table * slow_dims
    top_score = jax.random.uniform(jax.random.fold_in(plan_key, 6), block_shape, jnp.float32, 68.0, 80.0)
    score_gap = jax.random.uniform(jax.random.fold_in(plan_key, 7), block_shape, jnp.float32, 3.0, 8.0)
    head_root = math.sqrt(HD)
    scale_query = jnp.sqrt(2.0 * top_score / head_root)
    own_score = jnp.where(own_higher, top_score, top_score - score_gap)
    prev_score = jnp.where(own_higher, top_score - score_gap, top_score)
    own_level = own_score / (scale_query * head_root / 2.0)
    prev_level = prev_score / (scale_query * head_root / 2.0)
    return (own_hit, prev_hit, which_query, pattern, slow_dims, scale_query, own_level, prev_level)


def draw_key_heads(key, part):
    own_hit, prev_hit, which_query, pattern, slow_dims, scale_query, own_level, prev_level = aligned_plan(key)
    filler = background(jax.random.fold_in(key, 31), (NBLK, BLOCK, KVH, HD))
    key_level = jnp.where(own_hit, own_level, prev_level)
    aligned = key_level[..., None] * pattern + filler * (1.0 - slow_dims)
    hit_any = own_hit | prev_hit
    values = jnp.where(hit_any[..., None], aligned, filler)
    return values.reshape(LENGTH, KVH * HD).astype(jnp.bfloat16)


def draw_queries(key, part):
    own_hit, prev_hit, which_query, pattern, slow_dims, scale_query, own_level, prev_level = aligned_plan(key)
    filler = background(jax.random.fold_in(key, 37), (NBLK, BLOCK, H, HD))
    head_parity = (jnp.arange(H, dtype=jnp.int32) % 2)[None, None, :]
    query_hit = jnp.repeat(own_hit, 2, axis=2) & (jnp.repeat(which_query, 2, axis=2) == head_parity)
    pattern_heads = jnp.repeat(pattern, 2, axis=2)
    scale_heads = jnp.repeat(scale_query, 2, axis=2)
    aligned = scale_heads[..., None] * pattern_heads
    values = jnp.where(query_hit[..., None], aligned, filler)
    return values.reshape(LENGTH, H * HD).astype(jnp.bfloat16)


def steps_of(key, extent, pieces, low, high):
    level = 1.0
    for axis_at, shards_of in pieces:
        draws = jax.random.uniform(jax.random.fold_in(jax.random.fold_in(key, 6), axis_at), (shards_of,), jnp.float32, low / len(pieces), high / len(pieces))
        level = level * jnp.repeat(jnp.exp(draws), extent[axis_at] // shards_of).reshape((-1,) + (1,) * (len(extent) - 1 - axis_at))
    return level


def length_profile(number_of, total, most, lean):
    portions = [(1 << 20) // math.isqrt(standing ** lean) + 1 for standing in range(2, number_of + 1)]
    spare, given = total - most - (number_of - 1), [1] * (number_of - 1)
    while spare > 0:
        free = [i for i in range(number_of - 1) if given[i] < most]
        pool, left = sum([portions[i] for i in free]), spare
        for i in free:
            more = min(most - given[i], max(1, left * portions[i] // pool), spare)
            given[i] = given[i] + more
            spare = spare - more
    return np.array([most] + given)


def ragged_sizes(own_key, number_of, total, most, lean):
    if number_of == 2:
        one = jax.random.randint(own_key, (), max(1, total - most), min(most, total - 1) + 1)
        return jnp.stack([one, total - one])
    tallies = jnp.asarray(length_profile(number_of, total, most, lean), jnp.int32)
    twos = (number_of - 1) // 2
    source_of, taker = tallies[1:1 + 2 * twos:2], tallies[2:2 + 2 * twos:2]
    room = jnp.minimum(source_of - 1, most - taker)
    moved = jax.random.randint(jax.random.fold_in(own_key, 1), (twos,), 0, 1 << 20) % (room + 1)
    tallies = tallies.at[1:1 + 2 * twos:2].set(source_of - moved).at[2:2 + 2 * twos:2].set(taker + moved)
    return tallies[jax.random.permutation(jax.random.fold_in(own_key, 2), number_of)]


def bell_draw(stream_key, dims, scale, reach, split=(), kind=jnp.bfloat16):
    array = jax.random.normal(stream_key, dims, jnp.float32) * scale
    if len(split) > 0:
        array = steps_of(stream_key, dims, split, -0.22, 0.18) * array
    return jnp.clip(array, min=-reach, max=reach).astype(kind)


def setup_inputs(seed: int = 0, part: int = 0) -> dict:
    seeds = jax.random.split(jax.random.key(seed), 11)
    part_keys = jax.random.split(jax.random.fold_in(seeds[10], part), 11)
    return {
        "residual": bell_draw(part_keys[0], (LENGTH, D), 1.0, 6.0, ((0, 256),)),
        "queries": draw_queries(jax.random.fold_in(jax.random.fold_in(seeds[10], part), 71), part),
        "key_heads": draw_key_heads(jax.random.fold_in(jax.random.fold_in(seeds[10], part), 71), part),
        "value_heads": bell_draw(part_keys[3], (LENGTH, KVH * HD), 1.0, 6.0, ((0, 16), (1, 16))),
        "doc_blocks": ragged_sizes(part_keys[4], DOCS, NBLK, MOST_BLK, 2).astype(jnp.int32),
        "out_weight": draw_out_weight(jax.random.fold_in(seeds[10], 71), part),
        "post_gain": jnp.clip(1.0 + 0.18 * jax.random.normal(seeds[6], (D,), jnp.float32), 0.1, 1.9),
        "ffn_gain": jnp.clip(1.0 + 0.18 * jax.random.normal(seeds[7], (D,), jnp.float32), 0.1, 1.9),
        "gate_weight": bell_draw(seeds[8], (D, FF), D ** -0.5, 0.09375, ((0, 16), (1, 16))),
        "up_weight": bell_draw(seeds[9], (D, FF), D ** -0.5, 0.09375, ((0, 16), (1, 16))),
    }


SOFT_CAP = 50.0
NORM_EPS = 1e-06
ROPE_BASE = 10000.0

def rope_angles(positions, head_size):
    halfway = head_size // 2
    frequency = ROPE_BASE ** (-(jnp.arange(halfway, dtype=jnp.float32) * 2.0) / head_size)
    angles = positions.astype(jnp.float32)[:, None] * frequency[None, :]
    return (jnp.cos(angles), jnp.sin(angles))

def rotate(heads_in, cosine, sine_value, head_size):
    rows_here = heads_in.shape[0]
    reshaped = heads_in.astype(jnp.float32).reshape(rows_here, -1, head_size)
    leading = reshaped[:, :, :head_size // 2]
    trailing = reshaped[:, :, head_size // 2:]
    cos_wide = cosine[:, None, :]
    sin_wide = sine_value[:, None, :]
    turned = jnp.concatenate([leading * cos_wide - trailing * sin_wide, trailing * cos_wide + leading * sin_wide], axis=2)
    return turned.reshape(rows_here, -1).astype(jnp.bfloat16)

def doc_of(positions, doc_blocks):
    doc_ends = jnp.cumsum(doc_blocks)
    passed = positions[:, None] // BLOCK >= doc_ends[None, :]
    return lax.optimization_barrier(jnp.sum(passed.astype(jnp.int32), axis=1)).astype(jnp.int32)

def rms_scale(values):
    return values * lax.rsqrt(lax.optimization_barrier(jnp.mean(values * values, axis=-1, keepdims=True)) + NORM_EPS)

def gelu_gate(gate_sum, up_sum):
    return (jax.nn.gelu(gate_sum, approximate=True) * up_sum).astype(jnp.bfloat16)

def attend(running, query_rows, query_pos, query_doc, key_rows, value_rows, key_pos, key_doc, score_scale):
    scores = lax.dot_general(query_rows, key_rows, (((1,), (1,)), ((), ())), preferred_element_type=jnp.float32) * score_scale
    capped = SOFT_CAP * jnp.tanh(scores / SOFT_CAP)
    visible = (key_pos[None, :] <= query_pos[:, None]) & (key_doc[None, :] == query_doc[:, None])
    weights = jnp.where(visible, jnp.exp(capped), 0.0).astype(jnp.bfloat16)
    numerator = running[0] + jnp.dot(weights, value_rows, preferred_element_type=jnp.float32)
    denominator = running[1] + lax.optimization_barrier(jnp.sum(weights.astype(jnp.float32), axis=1))
    return (numerator, denominator)

def reference(residual, queries, key_heads, value_heads, doc_blocks, out_weight, post_gain, ffn_gain, gate_weight, up_weight):
    length = residual.shape[0]
    positions = jnp.arange(length, dtype=jnp.int32)
    doc_ids = doc_of(positions, doc_blocks)
    cosine, sine_value = rope_angles(positions, HD)
    query_rot = rotate(queries, cosine, sine_value, HD).reshape(length, H, HD)
    key_rot = rotate(key_heads, cosine, sine_value, HD).reshape(length, KVH, HD)
    value_split = value_heads.reshape(length, KVH, HD)
    weight_split = out_weight.reshape(H, HD, D)
    score_scale = HD ** (-0.5)

    def one_head(summed, head_index):
        query_head = lax.dynamic_index_in_dim(query_rot, head_index, 1, keepdims=False)
        key_head = lax.dynamic_index_in_dim(key_rot, head_index // 2, 1, keepdims=False)
        value_head = lax.dynamic_index_in_dim(value_split, head_index // 2, 1, keepdims=False)

        def one_block(block_args):
            query_rows, query_pos, query_doc = block_args
            empty_sums = (jnp.zeros((TOK_CTX, HD), jnp.float32), jnp.zeros((TOK_CTX,), jnp.float32))
            numerator, denominator = attend(empty_sums, query_rows, query_pos, query_doc, key_head, value_head, positions, doc_ids, score_scale)
            return (numerator / denominator[:, None]).astype(jnp.bfloat16)
        attended = lax.map(one_block, (query_head.reshape(-1, TOK_CTX, HD), positions.reshape(-1, TOK_CTX), doc_ids.reshape(-1, TOK_CTX)))
        attended = attended.reshape(length, HD)
        head_weight = lax.dynamic_index_in_dim(weight_split, head_index, 0, keepdims=False)
        head_term = jnp.dot(attended, head_weight, preferred_element_type=jnp.float32).astype(jnp.bfloat16)
        head_term = lax.optimization_barrier(head_term)
        return (summed + head_term.astype(jnp.float32), None)
    attn_sum, _ = lax.scan(one_head, jnp.zeros((length, D), jnp.float32), jnp.arange(H, dtype=jnp.int32))
    mixed_stream = (residual.astype(jnp.float32) + rms_scale(attn_sum) * post_gain).astype(jnp.bfloat16)
    ffn_input = (rms_scale(mixed_stream.astype(jnp.float32)) * ffn_gain).astype(jnp.bfloat16)
    gate_sum = jnp.dot(ffn_input, gate_weight, preferred_element_type=jnp.float32)
    up_sum = jnp.dot(ffn_input, up_weight, preferred_element_type=jnp.float32)
    ffn_hidden = gelu_gate(gate_sum, up_sum)
    return (mixed_stream, ffn_hidden)
```

```python
import functools

import jax
import jax.numpy as jnp
import numpy as np
from jax import lax
from jax.experimental import pallas as pl
from jax.experimental.pallas import tpu as pltpu
from jax.sharding import PartitionSpec as P

MESH = pl.DeviceIdType.MESH
BLOCK = 32
SOFT_CAP = 50.0
NORM_EPS = 1e-06
ROPE_BASE = 10000.0
RING = 16
TOK = 256
HEAD = 256
HALF = 128
WIDTH = 3584
ROWS = 16
SUBS = 4
SUB = WIDTH // SUBS
F32 = jnp.float32
BF16 = jnp.bfloat16


def rope_tables():
    freq = ROPE_BASE ** (-(np.arange(HALF, dtype=np.float64) * 2.0) / HEAD)
    inner = np.arange(TOK, dtype=np.float64)[:, None] * freq[None, :]
    outer = (np.arange(16, dtype=np.float64) * TOK)[:, None] * freq[None, :]
    return tuple(np.asarray(f(a), np.float32) for a in (inner, outer) for f in (np.cos, np.sin))


class Sends:
    def __init__(self):
        self.pending = []

    def go(self, copy, cond=None):
        if cond is None:
            copy.start()
        else:
            pl.when(cond)(copy.start)
        self.pending.append((copy, cond))

    def drain(self):
        for copy, cond in self.pending:
            if cond is None:
                copy.wait_send()
            else:
                pl.when(cond)(copy.wait_send)
        self.pending = []


def layer_kernel(
    q_ref,
    k_ref,
    v_ref,
    doc_ref,
    res_ref,
    post_ref,
    ffn_ref,
    cos_in,
    sin_in,
    cos_out,
    sin_out,
    ow_hbm,
    mixed_ref,
    x_out,
    ow,
    rawk,
    kk,
    vv,
    qrot,
    num,
    den,
    term,
    rs_r,
    rs_l,
    acc,
    x_buf,
    ow_sem,
    pair_send,
    pair_recv,
    kv_send,
    k_recv,
    v_recv,
    rs_send,
    rs_recv,
    ag_send,
    ag_recv,
):
    dp = lax.axis_index("dp")
    c = lax.axis_index("ctx")
    t = lax.axis_index("tensor")
    row = c // 8
    x = (c % 8) // 2
    core = c % 2
    par = t % 2

    def at(r, xx, kk_, d=dp):
        return (d, r * 8 + xx * 2 + kk_, t)

    x_up = (x + 1) % 4
    x_dn = (x + 3) % 4
    right_x = at(row, x_up, core)
    left_x = at(row, x_dn, core)
    cross = at(1 - row, x, core)
    sib = at(row, x, 1 - core)
    z_up = (dp, c, (t + 1) % RING)
    z_dn = (dp, c, (t + RING - 1) % RING)
    mate = (dp, c, t + 1 - 2 * par)

    barrier = pltpu.get_barrier_semaphore()
    friends = (right_x, left_x, cross, sib, z_up, z_dn)
    for friend in friends:
        pl.semaphore_signal(barrier, inc=1, device_id=friend, device_id_type=MESH)
    ow_copy = pltpu.make_async_copy(ow_hbm, ow, ow_sem)
    ow_copy.start()

    sends = Sends()

    def remote(src, dst, send, recv, to):
        return pltpu.make_async_remote_copy(
            src_ref=src, dst_ref=dst, send_sem=send, recv_sem=recv, device_id=to, device_id_type=MESH
        )

    own_lanes = pl.ds(pl.multiple_of(par * HALF, HALF), HALF)
    pl.semaphore_wait(barrier, len(friends))
    pair_k = remote(k_ref, rawk.at[par], pair_send.at[0], pair_recv.at[0], mate)
    pair_v = remote(v_ref, vv.at[c, :, own_lanes], pair_send.at[1], pair_recv.at[1], mate)
    sends.go(pair_k)
    sends.go(pair_v)

    cb = cos_out[pl.ds(c, 1), :]
    sb = sin_out[pl.ds(c, 1), :]
    cosine = cos_in[...] * cb - sin_in[...] * sb
    sine = sin_in[...] * cb + cos_in[...] * sb

    def turned(a, b, where):
        a, b = a.astype(F32), b.astype(F32)
        where[:, :HALF] = (a * cosine - b * sine).astype(BF16)
        where[:, HALF:] = (b * cosine + a * sine).astype(BF16)

    turned(q_ref[:, :HALF], q_ref[:, HALF:], qrot)
    rawk[par] = k_ref[...]
    vv[c, :, own_lanes] = v_ref[...]
    num[...] = jnp.zeros_like(num)
    den[...] = jnp.zeros_like(den)

    qpos = c * TOK + lax.broadcasted_iota(jnp.int32, (TOK, 1), 0)
    begin = jnp.zeros((TOK, 1), jnp.int32)
    total = 0
    for e in range(5):
        total = total + doc_ref[e]
        edge = total * BLOCK
        begin = jnp.where(qpos >= edge, jnp.maximum(begin, edge), begin)

    def attend(b):
        lane = b * TOK + lax.broadcasted_iota(jnp.int32, (1, TOK), 1)
        scores = lax.dot_general(
            qrot[...], kk[b], (((1,), (1,)), ((), ())), preferred_element_type=F32
        )
        capped = jnp.tanh(scores * (1.0 / (SOFT_CAP * HEAD**0.5))) * (SOFT_CAP / np.log(2.0))
        visible = (lane >= begin) & (lane <= qpos)
        weights = jnp.where(visible, jnp.exp2(capped), 0.0).astype(BF16)
        wide = weights.astype(F32)
        den[...] += wide[:, :HALF] + wide[:, HALF:]
        num[...] += jnp.dot(weights, vv[b], preferred_element_type=F32)

    slot = iter(range(64))

    def k_copy(b, to):
        return remote(kk.at[b], kk.at[b], kv_send.at[next(slot)], k_recv.at[b], to)

    def v_copy(b, to):
        return remote(vv.at[b], vv.at[b], kv_send.at[next(slot)], v_recv.at[b], to)

    def k_wait(b, cond):
        got = remote(kk.at[b], kk.at[b], kv_send.at[0], k_recv.at[b], sib)
        pl.when(cond)(got.wait_recv)

    def v_wait(b, cond):
        got = remote(vv.at[b], vv.at[b], kv_send.at[0], v_recv.at[b], sib)
        pl.when(cond)(got.wait_recv)

    pair_k.wait_recv()
    turned(rawk[0], rawk[1], kk.at[c])

    def spread(copy):
        sends.go(copy(c, right_x), x < 3)
        sends.go(copy(c, left_x), x == 0)
        sends.go(copy(c, cross), row == 0)
        sends.go(copy(c, sib), core == 0)

    spread(k_copy)
    pair_v.wait_recv()
    spread(v_copy)
    attend(c)

    mid = (x == 1) | (x == 2)
    lower = row == 1
    for hop in (1, 2, 3):
        b = jnp.maximum(c - 2 * hop, 0)
        here = x >= hop
        for wait, copy in ((k_wait, k_copy), (v_wait, v_copy)):
            wait(b, here)
            if hop == 1:
                sends.go(copy(b, right_x), mid)
            sends.go(copy(b, sib), here)
        if hop == 1:
            own0 = jnp.maximum(c - 8, 0)
            for wait, copy in ((k_wait, k_copy), (v_wait, v_copy)):
                wait(own0, lower)
                sends.go(copy(own0, left_x), lower & (x > 0))
                sends.go(copy(own0, right_x), lower & (x == 3))
                sends.go(copy(own0, sib), lower & (core == 1))
    for hop in (1, 2, 3):
        b = jnp.clip(c - 8 + 2 * hop, 0, 15)
        here = lower & (x + hop <= 3)
        for wait, copy in ((k_wait, k_copy), (v_wait, v_copy)):
            wait(b, here)
            if hop == 1:
                sends.go(copy(b, left_x), lower & mid)
            sends.go(copy(b, sib), here)

    first = jnp.maximum(c - 8, 0)

    def visit(b, carry):
        other = (b % 2) != core
        k_wait(b, other)
        v_wait(b, other)
        attend(b)
        return carry

    lax.fori_loop(first, c, visit, 0)
    ow_copy.wait()

    sums = jnp.sum(den[...], axis=1, keepdims=True)
    attended = (num[...] / sums).astype(BF16)

    def lanes(s):
        return pl.ds(s * SUB, SUB)

    def block(d):
        return pl.ds(pl.multiple_of(lax.rem(t + d + RING, RING) * ROWS, ROWS), ROWS)

    HOPS = RING // 2
    flows = (
        (0, rs_r, z_up, 1, (0, 1)),
        (1, rs_l, z_dn, -1, (2, 3)),
    )

    def rs_step(k, s):
        for f, buf, to, sign, early in flows:
            begin_at = 1 if s in early else 2
            if k < begin_at:
                continue
            away = sign * (HOPS + 1 - k)
            if k == begin_at:
                src = term.at[block(away), lanes(s)]
            else:
                src = buf.at[k - 2, :, lanes(s)]
                remote(src, src, rs_send.at[f, k - 2, s], rs_recv.at[f, k - 2, s], to).wait_recv()
                buf[k - 2, :, lanes(s)] = (
                    buf[k - 2, :, lanes(s)].astype(F32) + term[block(away), lanes(s)].astype(F32)
                ).astype(BF16)
            sends.go(
                remote(src, buf.at[k - 1, :, lanes(s)], rs_send.at[f, k - 1, s], rs_recv.at[f, k - 1, s], to)
            )

    for s in range(SUBS):
        term[:, lanes(s)] = jnp.dot(attended, ow[:, lanes(s)], preferred_element_type=F32).astype(BF16)
        rs_step(1, s)
    for k in range(2, HOPS + 1):
        for s in range(SUBS):
            rs_step(k, s)

    square = jnp.zeros((ROWS, 1), F32)
    for s in range(SUBS):
        for f, buf, to, _, _ in flows:
            src = buf.at[HOPS - 1, :, lanes(s)]
            remote(src, src, rs_send.at[f, HOPS - 1, s], rs_recv.at[f, HOPS - 1, s], to).wait_recv()
        part = (
            term[block(0), lanes(s)].astype(F32)
            + rs_r[HOPS - 1, :, lanes(s)].astype(F32)
            + rs_l[HOPS - 1, :, lanes(s)].astype(F32)
        )
        acc[:, lanes(s)] = part
        square += jnp.sum(part * part, axis=1, keepdims=True)
    scale = lax.rsqrt(square / WIDTH + NORM_EPS)
    mixed = (res_ref[...].astype(F32) + acc[...] * scale * post_ref[...]).astype(BF16)
    mixed_ref[...] = mixed
    wide = mixed.astype(F32)
    scale = lax.rsqrt(jnp.sum(wide * wide, axis=1, keepdims=True) / WIDTH + NORM_EPS)
    x_buf[block(0), :] = (wide * scale * ffn_ref[...]).astype(BF16)

    ag_flows = ((0, z_up, -1, (0, 1)), (1, z_dn, 1, (2, 3)))

    def ag_got(k, s):
        for f, to, sign, late in ag_flows:
            if k == HOPS and s not in late:
                continue
            src = x_buf.at[block(sign * k), lanes(s)]
            remote(src, src, ag_send.at[f, k - 1, s], ag_recv.at[f, k - 1, s], to).wait_recv()

    for k in range(1, HOPS + 1):
        for s in range(SUBS):
            for f, to, sign, late in ag_flows:
                if k > 1:
                    got = x_buf.at[block(sign * (k - 1)), lanes(s)]
                    remote(got, got, ag_send.at[f, k - 2, s], ag_recv.at[f, k - 2, s], to).wait_recv()
                if k == HOPS and s not in late:
                    continue
                src = x_buf.at[block(sign * (k - 1)), lanes(s)]
                sends.go(remote(src, src, ag_send.at[f, k - 1, s], ag_recv.at[f, k - 1, s], to))
    for s in range(SUBS):
        ag_got(HOPS, s)
    x_out[...] = x_buf[...]
    sends.drain()


def attention_half(q, k, v, doc_blocks, residual, post_gain, ffn_gain, out_weight):
    vmem = pl.BlockSpec(memory_space=pltpu.VMEM)
    tables = [jnp.asarray(a) for a in rope_tables()]
    half = RING // 2
    dma = pltpu.SemaphoreType.DMA
    return pl.pallas_call(
        layer_kernel,
        out_shape=(
            jax.ShapeDtypeStruct((ROWS, WIDTH), BF16),
            jax.ShapeDtypeStruct((TOK, WIDTH), BF16),
        ),
        in_specs=[vmem] * 3
        + [pl.BlockSpec(memory_space=pltpu.SMEM)]
        + [vmem] * 7
        + [pl.BlockSpec(memory_space=pl.ANY)],
        out_specs=(vmem, vmem),
        scratch_shapes=[
            pltpu.VMEM((HEAD, WIDTH), BF16),
            pltpu.VMEM((2, TOK, HALF), BF16),
            pltpu.VMEM((16, TOK, HEAD), BF16),
            pltpu.VMEM((16, TOK, HEAD), BF16),
            pltpu.VMEM((TOK, HEAD), BF16),
            pltpu.VMEM((TOK, HEAD), F32),
            pltpu.VMEM((TOK, HALF), F32),
            pltpu.VMEM((TOK, WIDTH), BF16),
            pltpu.VMEM((half, ROWS, WIDTH), BF16),
            pltpu.VMEM((half, ROWS, WIDTH), BF16),
            pltpu.VMEM((ROWS, WIDTH), F32),
            pltpu.VMEM((TOK, WIDTH), BF16),
            dma,
            dma((2,)),
            dma((2,)),
            dma((40,)),
            dma((16,)),
            dma((16,)),
            dma((2, half, SUBS)),
            dma((2, half, SUBS)),
            dma((2, half, SUBS)),
            dma((2, half, SUBS)),
        ],
        compiler_params=pltpu.CompilerParams(
            collective_id=0, has_side_effects=True, vmem_limit_bytes=48 * 1024 * 1024
        ),
        cost_estimate=pl.CostEstimate(flops=2_000_000_000, bytes_accessed=8_000_000, transcendentals=0),
    )(
        q,
        k,
        v,
        doc_blocks,
        residual,
        post_gain.reshape(1, WIDTH),
        ffn_gain.reshape(1, WIDTH),
        *tables,
        out_weight,
    )


def gelu_gate(gate_sum, up_sum):
    return (jax.nn.gelu(gate_sum, approximate=True) * up_sum).astype(BF16)


def per_device(
    residual,
    queries,
    key_heads,
    value_heads,
    doc_blocks,
    out_weight,
    post_gain,
    ffn_gain,
    gate_weight,
    up_weight,
):
    both = jnp.concatenate([gate_weight, up_weight], axis=1)
    whole = lax.all_gather(both, "ctx", axis=0, tiled=True)
    mixed_stream, rows = attention_half(
        queries, key_heads, value_heads, doc_blocks, residual, post_gain, ffn_gain, out_weight
    )
    columns = gate_weight.shape[1]
    gate_part = jnp.dot(rows, whole[:, :columns], preferred_element_type=F32)
    up_part = jnp.dot(rows, whole[:, columns:], preferred_element_type=F32)
    return (mixed_stream, gelu_gate(gate_part, up_part))


def solution(mesh):
    in_specs = (
        P(("dp", "ctx", "tensor"), None),
        P(("dp", "ctx"), "tensor"),
        P(("dp", "ctx"), "tensor"),
        P(("dp", "ctx"), "tensor"),
        P("dp"),
        P("tensor", None),
        P(),
        P(),
        P("ctx", "tensor"),
        P("ctx", "tensor"),
    )
    out_specs = (P(("dp", "ctx", "tensor"), None), P(("dp", "ctx"), "tensor"))
    return jax.shard_map(
        per_device, mesh=mesh, in_specs=in_specs, out_specs=out_specs, check_vma=False
    )
```

```python
import functools

import jax
import jax.numpy as jnp
import numpy as np
from jax import lax
from jax.experimental import pallas as pl
from jax.experimental.pallas import tpu as pltpu
from jax.sharding import PartitionSpec as P

MESH = pl.DeviceIdType.MESH
BLOCK = 32
SOFT_CAP = 50.0
NORM_EPS = 1e-06
ROPE_BASE = 10000.0
RING = 16
TOK = 256
HEAD = 256
HALF = 128
WIDTH = 3584
ROWS = 16
SUBS = 4
SUB = WIDTH // SUBS
SHARD = 224
COLS = 896
TILES = COLS // 128
MAIN = 144
REST = SHARD - MAIN
NEAR = 80
FAR = MAIN - NEAR
F32 = jnp.float32
BF16 = jnp.bfloat16


def rope_tables():
    freq = ROPE_BASE ** (-(np.arange(HALF, dtype=np.float64) * 2.0) / HEAD)
    inner = np.arange(TOK, dtype=np.float64)[:, None] * freq[None, :]
    outer = (np.arange(16, dtype=np.float64) * TOK)[:, None] * freq[None, :]
    return tuple(np.asarray(f(a), np.float32) for a in (inner, outer) for f in (np.cos, np.sin))


class Sends:
    def __init__(self):
        self.pending = []

    def go(self, copy, cond=None):
        if cond is None:
            copy.start()
        else:
            pl.when(cond)(copy.start)
        self.pending.append((copy, cond))

    def drain(self):
        for copy, cond in self.pending:
            if cond is None:
                copy.wait_send()
            else:
                pl.when(cond)(copy.wait_send)
        self.pending = []


def layer_kernel(
    q_ref,
    k_ref,
    v_ref,
    doc_ref,
    res_ref,
    post_ref,
    ffn_ref,
    cos_in,
    sin_in,
    cos_out,
    sin_out,
    ow_hbm,
    gate_hbm,
    up_hbm,
    mixed_ref,
    hidden_ref,
    ow,
    w,
    rawk,
    kk,
    vv,
    qrot,
    num,
    den,
    term,
    rs_r,
    rs_l,
    acc,
    x_buf,
    ow_sem,
    pair_send,
    pair_recv,
    kv_send,
    k_recv,
    v_recv,
    rs_send,
    rs_recv,
    ag_send,
    ag_recv,
    w_load,
    w_send,
    w_recv,
):
    dp = lax.axis_index("dp")
    c = lax.axis_index("ctx")
    t = lax.axis_index("tensor")
    row = c // 8
    x = (c % 8) // 2
    core = c % 2
    par = t % 2

    def at(r, xx, kk_, d=dp):
        return (d, r * 8 + xx * 2 + kk_, t)

    x_up = (x + 1) % 4
    x_dn = (x + 3) % 4
    right_x = at(row, x_up, core)
    left_x = at(row, x_dn, core)
    cross = at(1 - row, x, core)
    sib = at(row, x, 1 - core)
    z_up = (dp, c, (t + 1) % RING)
    z_dn = (dp, c, (t + RING - 1) % RING)
    mate = (dp, c, t + 1 - 2 * par)
    twin = at(row, x, core, 1 - dp)
    other = at(1 - row, x, core, 1 - dp)

    barrier = pltpu.get_barrier_semaphore()
    friends = (right_x, left_x, cross, sib, z_up, z_dn, twin, other)
    for friend in friends:
        pl.semaphore_signal(barrier, inc=1, device_id=friend, device_id_type=MESH)
    ow_copy = pltpu.make_async_copy(ow_hbm, ow, ow_sem)
    ow_copy.start()
    own_rows = pl.ds(pl.multiple_of(c * SHARD, 16), SHARD)
    loads = []
    for n in range(TILES):
        for i, ref in enumerate((gate_hbm, up_hbm)):
            loads.append(
                pltpu.make_async_copy(
                    ref.at[:, pl.ds(n * 128, 128)],
                    w.at[own_rows, pl.ds(n * 256 + i * 128, 128)],
                    w_load.at[n, i],
                )
            )
    for load in loads:
        load.start()

    sends = Sends()

    def remote(src, dst, send, recv, to):
        return pltpu.make_async_remote_copy(
            src_ref=src, dst_ref=dst, send_sem=send, recv_sem=recv, device_id=to, device_id_type=MESH
        )

    own_lanes = pl.ds(pl.multiple_of(par * HALF, HALF), HALF)
    pl.semaphore_wait(barrier, len(friends))
    pair_k = remote(k_ref, rawk.at[par], pair_send.at[0], pair_recv.at[0], mate)
    pair_v = remote(v_ref, vv.at[c, :, own_lanes], pair_send.at[1], pair_recv.at[1], mate)
    sends.go(pair_k)
    sends.go(pair_v)

    cb = cos_out[pl.ds(c, 1), :]
    sb = sin_out[pl.ds(c, 1), :]
    cosine = cos_in[...] * cb - sin_in[...] * sb
    sine = sin_in[...] * cb + cos_in[...] * sb

    def turned(a, b, where):
        a, b = a.astype(F32), b.astype(F32)
        where[:, :HALF] = (a * cosine - b * sine).astype(BF16)
        where[:, HALF:] = (b * cosine + a * sine).astype(BF16)

    turned(q_ref[:, :HALF], q_ref[:, HALF:], qrot)
    rawk[par] = k_ref[...]
    vv[c, :, own_lanes] = v_ref[...]
    num[...] = jnp.zeros_like(num)
    den[...] = jnp.zeros_like(den)

    qpos = c * TOK + lax.broadcasted_iota(jnp.int32, (TOK, 1), 0)
    begin = jnp.zeros((TOK, 1), jnp.int32)
    total = 0
    for e in range(5):
        total = total + doc_ref[e]
        edge = total * BLOCK
        begin = jnp.where(qpos >= edge, jnp.maximum(begin, edge), begin)

    def attend(b):
        lane = b * TOK + lax.broadcasted_iota(jnp.int32, (1, TOK), 1)
        scores = lax.dot_general(
            qrot[...], kk[b], (((1,), (1,)), ((), ())), preferred_element_type=F32
        )
        capped = jnp.tanh(scores * (1.0 / (SOFT_CAP * HEAD**0.5))) * (SOFT_CAP / np.log(2.0))
        visible = (lane >= begin) & (lane <= qpos)
        weights = jnp.where(visible, jnp.exp2(capped), 0.0).astype(BF16)
        wide = weights.astype(F32)
        den[...] += wide[:, :HALF] + wide[:, HALF:]
        num[...] += jnp.dot(weights, vv[b], preferred_element_type=F32)

    slot = iter(range(64))

    def k_copy(b, to):
        return remote(kk.at[b], kk.at[b], kv_send.at[next(slot)], k_recv.at[b], to)

    def v_copy(b, to):
        return remote(vv.at[b], vv.at[b], kv_send.at[next(slot)], v_recv.at[b], to)

    def k_wait(b, cond):
        got = remote(kk.at[b], kk.at[b], kv_send.at[0], k_recv.at[b], sib)
        pl.when(cond)(got.wait_recv)

    def v_wait(b, cond):
        got = remote(vv.at[b], vv.at[b], kv_send.at[0], v_recv.at[b], sib)
        pl.when(cond)(got.wait_recv)

    pair_k.wait_recv()
    turned(rawk[0], rawk[1], kk.at[c])

    def spread(copy):
        sends.go(copy(c, right_x), x < 3)
        sends.go(copy(c, left_x), x == 0)
        sends.go(copy(c, cross), row == 0)
        sends.go(copy(c, sib), core == 0)

    spread(k_copy)
    pair_v.wait_recv()
    spread(v_copy)
    attend(c)

    mid = (x == 1) | (x == 2)
    lower = row == 1
    for hop in (1, 2, 3):
        b = jnp.maximum(c - 2 * hop, 0)
        here = x >= hop
        for wait, copy in ((k_wait, k_copy), (v_wait, v_copy)):
            wait(b, here)
            if hop == 1:
                sends.go(copy(b, right_x), mid)
            sends.go(copy(b, sib), here)
        if hop == 1:
            own0 = jnp.maximum(c - 8, 0)
            for wait, copy in ((k_wait, k_copy), (v_wait, v_copy)):
                wait(own0, lower)
                sends.go(copy(own0, left_x), lower & (x > 0))
                sends.go(copy(own0, right_x), lower & (x == 3))
                sends.go(copy(own0, sib), lower & (core == 1))
    for hop in (1, 2, 3):
        b = jnp.clip(c - 8 + 2 * hop, 0, 15)
        here = lower & (x + hop <= 3)
        for wait, copy in ((k_wait, k_copy), (v_wait, v_copy)):
            wait(b, here)
            if hop == 1:
                sends.go(copy(b, left_x), lower & mid)
            sends.go(copy(b, sib), here)

    w_slot = iter(range(64))

    def shard(r, dx, plane=core):
        return r * 8 + ((x + dx) % 4) * 2 + plane

    def cut(b, start, size):
        return w.at[pl.ds(pl.multiple_of(b * SHARD + start, 16), size), :]

    def w_go(b, start, size, kind, to):
        ref = cut(b, start, size)
        sends.go(remote(ref, ref, w_send.at[next(w_slot)], w_recv.at[b, kind], to))

    def w_wait(b, size, kind):
        ref = cut(b, 0, size)
        remote(ref, ref, w_send.at[0], w_recv.at[b, kind], sib).wait_recv()

    main_at = REST * dp
    rest_at = MAIN * dp
    twin_main_at = REST * (1 - dp)
    twin_rest_at = MAIN * (1 - dp)

    def w_first():
        for load in loads:
            load.wait()
        b = shard(row, 0)
        w_go(b, twin_main_at, MAIN, 0, other)
        w_go(b, main_at, MAIN, 0, right_x)
        w_go(b, main_at, MAIN, 0, left_x)
        w_go(b, rest_at, REST, 1, other)
        w_go(b, 0, SHARD, 0, sib)

    def w_cross():
        b = shard(1 - row, 0)
        w_wait(b, MAIN, 0)
        w_go(b, main_at, MAIN, 0, right_x)
        w_go(b, main_at, MAIN, 0, left_x)
        w_go(b, main_at, MAIN, 0, sib)

    def w_cross_rest():
        b = shard(1 - row, 0)
        w_wait(b, REST, 1)
        w_go(b, twin_rest_at, REST, 1, sib)

    def w_next(r):
        for dx, to, start, size, kind in ((-1, right_x, 0, NEAR, 0), (1, left_x, NEAR, FAR, 2)):
            b = shard(r, dx)
            w_wait(b, MAIN, 0)
            w_go(b, main_at + start, size, kind, to)
            w_go(b, rest_at, REST, 1, at((row + r) % 2, x, core, 1 - dp))
            w_go(b, main_at, MAIN, 0, sib)

    def w_far(r):
        b = shard(r, 2)
        w_wait(b, NEAR, 0)
        w_wait(b, FAR, 2)
        w_go(b, rest_at, REST, 1, twin)
        w_go(b, main_at, MAIN, 0, sib)

    def w_rest(r, dx):
        b = shard(r, dx)
        w_wait(b, REST, 1)
        w_go(b, twin_rest_at, REST, 1, sib)

    def w_last():
        for r in (row, 1 - row):
            for dx in (0, -1, 1, 2):
                b = shard(r, dx, 1 - core)
                if dx == 0 and r is row:
                    w_wait(b, SHARD, 0)
                else:
                    w_wait(b, MAIN, 0)
                    w_wait(b, REST, 1)

    w_first()
    first = jnp.maximum(c - 8, 0)

    def visit(b, carry):
        other = (b % 2) != core
        k_wait(b, other)
        v_wait(b, other)
        attend(b)
        return carry

    lax.fori_loop(first, c, visit, 0)
    ow_copy.wait()

    sums = jnp.sum(den[...], axis=1, keepdims=True)
    attended = (num[...] / sums).astype(BF16)

    def lanes(s):
        return pl.ds(s * SUB, SUB)

    def block(d):
        return pl.ds(pl.multiple_of(lax.rem(t + d + RING, RING) * ROWS, ROWS), ROWS)

    HOPS = RING // 2
    flows = (
        (0, rs_r, z_up, 1, (0, 1)),
        (1, rs_l, z_dn, -1, (2, 3)),
    )

    def rs_step(k, s):
        for f, buf, to, sign, early in flows:
            begin_at = 1 if s in early else 2
            if k < begin_at:
                continue
            away = sign * (HOPS + 1 - k)
            if k == begin_at:
                src = term.at[block(away), lanes(s)]
            else:
                src = buf.at[k - 2, :, lanes(s)]
                remote(src, src, rs_send.at[f, k - 2, s], rs_recv.at[f, k - 2, s], to).wait_recv()
                buf[k - 2, :, lanes(s)] = (
                    buf[k - 2, :, lanes(s)].astype(F32) + term[block(away), lanes(s)].astype(F32)
                ).astype(BF16)
            sends.go(
                remote(src, buf.at[k - 1, :, lanes(s)], rs_send.at[f, k - 1, s], rs_recv.at[f, k - 1, s], to)
            )

    for s in range(SUBS):
        term[:, lanes(s)] = jnp.dot(attended, ow[:, lanes(s)], preferred_element_type=F32).astype(BF16)
        rs_step(1, s)
    for k in range(2, HOPS + 1):
        for s in range(SUBS):
            rs_step(k, s)
        if k == 4:
            w_next(row)
        if k == 5:
            w_cross()
        if k == 6:
            w_far(row)
        if k == 7:
            w_cross_rest()

    def whole_row(ref):
        return jnp.concatenate([ref[i : i + 1, :] for i in range(WIDTH // 128)], axis=1)

    square = jnp.zeros((ROWS, 1), F32)
    for s in range(SUBS):
        for f, buf, to, _, _ in flows:
            src = buf.at[HOPS - 1, :, lanes(s)]
            remote(src, src, rs_send.at[f, HOPS - 1, s], rs_recv.at[f, HOPS - 1, s], to).wait_recv()
        part = (
            term[block(0), lanes(s)].astype(F32)
            + rs_r[HOPS - 1, :, lanes(s)].astype(F32)
            + rs_l[HOPS - 1, :, lanes(s)].astype(F32)
        )
        acc[:, lanes(s)] = part
        square += jnp.sum(part * part, axis=1, keepdims=True)
    scale = lax.rsqrt(square / WIDTH + NORM_EPS)
    mixed = (res_ref[...].astype(F32) + acc[...] * scale * whole_row(post_ref)).astype(BF16)
    mixed_ref[...] = mixed
    wide = mixed.astype(F32)
    scale = lax.rsqrt(jnp.sum(wide * wide, axis=1, keepdims=True) / WIDTH + NORM_EPS)
    x_buf[block(0), :] = (wide * scale * whole_row(ffn_ref)).astype(BF16)

    ag_flows = ((0, z_up, -1, (0, 1)), (1, z_dn, 1, (2, 3)))

    def ag_got(k, s):
        for f, to, sign, late in ag_flows:
            if k == HOPS and s not in late:
                continue
            src = x_buf.at[block(sign * k), lanes(s)]
            remote(src, src, ag_send.at[f, k - 1, s], ag_recv.at[f, k - 1, s], to).wait_recv()

    for k in range(1, HOPS + 1):
        for s in range(SUBS):
            for f, to, sign, late in ag_flows:
                if k > 1:
                    got = x_buf.at[block(sign * (k - 1)), lanes(s)]
                    remote(got, got, ag_send.at[f, k - 2, s], ag_recv.at[f, k - 2, s], to).wait_recv()
                if k == HOPS and s not in late:
                    continue
                src = x_buf.at[block(sign * (k - 1)), lanes(s)]
                sends.go(remote(src, src, ag_send.at[f, k - 1, s], ag_recv.at[f, k - 1, s], to))
        if k == 2:
            w_next(1 - row)
        if k == 3:
            w_rest(row, -1)
            w_rest(row, 1)
        if k == 5:
            w_far(1 - row)
            w_rest(row, 2)
        if k == 7:
            w_rest(1 - row, -1)
            w_rest(1 - row, 1)
    for s in range(SUBS):
        ag_got(HOPS, s)
    w_rest(1 - row, 2)
    w_last()

    def column(n, carry):
        both = jnp.dot(
            x_buf[...], w[:, pl.ds(pl.multiple_of(n * 256, 256), 256)], preferred_element_type=F32
        )
        gate, up = both[:, :128], both[:, 128:]
        hidden_ref[:, pl.ds(pl.multiple_of(n * 128, 128), 128)] = (
            jax.nn.gelu(gate, approximate=True) * up
        ).astype(BF16)
        return carry

    lax.fori_loop(0, TILES, column, 0)
    sends.drain()


def layer(q, k, v, doc_blocks, residual, post_gain, ffn_gain, out_weight, gate, up):
    vmem = pl.BlockSpec(memory_space=pltpu.VMEM)
    tables = [jnp.asarray(a) for a in rope_tables()]
    half = RING // 2
    dma = pltpu.SemaphoreType.DMA
    return pl.pallas_call(
        layer_kernel,
        out_shape=(
            jax.ShapeDtypeStruct((ROWS, WIDTH), BF16),
            jax.ShapeDtypeStruct((TOK, COLS), BF16),
        ),
        in_specs=[vmem] * 3
        + [pl.BlockSpec(memory_space=pltpu.SMEM)]
        + [vmem] * 7
        + [pl.BlockSpec(memory_space=pl.ANY)] * 3,
        out_specs=(vmem, vmem),
        scratch_shapes=[
            pltpu.VMEM((HEAD, WIDTH), BF16),
            pltpu.VMEM((16 * SHARD, 2 * COLS), BF16),
            pltpu.VMEM((2, TOK, HALF), BF16),
            pltpu.VMEM((16, TOK, HEAD), BF16),
            pltpu.VMEM((16, TOK, HEAD), BF16),
            pltpu.VMEM((TOK, HEAD), BF16),
            pltpu.VMEM((TOK, HEAD), F32),
            pltpu.VMEM((TOK, HALF), F32),
            pltpu.VMEM((TOK, WIDTH), BF16),
            pltpu.VMEM((half, ROWS, WIDTH), BF16),
            pltpu.VMEM((half, ROWS, WIDTH), BF16),
            pltpu.VMEM((ROWS, WIDTH), F32),
            pltpu.VMEM((TOK, WIDTH), BF16),
            dma,
            dma((2,)),
            dma((2,)),
            dma((40,)),
            dma((16,)),
            dma((16,)),
            dma((2, half, SUBS)),
            dma((2, half, SUBS)),
            dma((2, half, SUBS)),
            dma((2, half, SUBS)),
            dma((TILES, 2)),
            dma((40,)),
            dma((16, 3)),
        ],
        compiler_params=pltpu.CompilerParams(
            collective_id=0, has_side_effects=True, vmem_limit_bytes=56 * 1024 * 1024
        ),
        cost_estimate=pl.CostEstimate(flops=2_000_000_000, bytes_accessed=8_000_000, transcendentals=0),
    )(
        q,
        k,
        v,
        doc_blocks,
        residual,
        post_gain.reshape(WIDTH // 128, 128),
        ffn_gain.reshape(WIDTH // 128, 128),
        *tables,
        out_weight,
        gate,
        up,
    )


def per_device(
    residual,
    queries,
    key_heads,
    value_heads,
    doc_blocks,
    out_weight,
    post_gain,
    ffn_gain,
    gate_weight,
    up_weight,
):
    return layer(
        queries,
        key_heads,
        value_heads,
        doc_blocks,
        residual,
        post_gain,
        ffn_gain,
        out_weight,
        gate_weight,
        up_weight,
    )


def solution(mesh):
    in_specs = (
        P(("dp", "ctx", "tensor"), None),
        P(("dp", "ctx"), "tensor"),
        P(("dp", "ctx"), "tensor"),
        P(("dp", "ctx"), "tensor"),
        P("dp"),
        P("tensor", None),
        P(),
        P(),
        P("ctx", "tensor"),
        P("ctx", "tensor"),
    )
    out_specs = (P(("dp", "ctx", "tensor"), None), P(("dp", "ctx"), "tensor"))
    return jax.shard_map(
        per_device, mesh=mesh, in_specs=in_specs, out_specs=out_specs, check_vma=False
    )
```

```python
import functools
import itertools

import jax
import jax.numpy as jnp
import numpy as np
from jax import lax
from jax.experimental import pallas as pl
from jax.experimental.pallas import tpu as pltpu
from jax.sharding import PartitionSpec as P

MESH = pl.DeviceIdType.MESH
BLOCK = 32
SOFT_CAP = 50.0
NORM_EPS = 1e-06
ROPE_BASE = 10000.0
RING = 16
TOK = 256
HEAD = 256
HALF = 128
WIDTH = 3584
ROWS = 16
SUBS = 4
SUB = WIDTH // SUBS
SHARD = 224
COLS = 896
TILES = COLS // 128
MAIN = 144
REST = SHARD - MAIN
POOL = 36
NEAR = 80
FAR = MAIN - NEAR
F32 = jnp.float32
BF16 = jnp.bfloat16


def rope_tables():
    freq = ROPE_BASE ** (-(np.arange(HALF, dtype=np.float64) * 2.0) / HEAD)
    inner = np.arange(TOK, dtype=np.float64)[:, None] * freq[None, :]
    outer = (np.arange(16, dtype=np.float64) * TOK)[:, None] * freq[None, :]
    return np.concatenate([f(a) for a in (inner, outer) for f in (np.cos, np.sin)]).astype(np.float32)


class Sends:
    def __init__(self):
        self.pending = {}

    @staticmethod
    def under(cond, act):
        if cond is None:
            act()
        else:
            pl.when(cond)(act)

    def go(self, key, copy, cond=None):
        self.settle(key)
        self.under(cond, copy.start)
        self.pending[key] = (copy, cond)

    def settle(self, key):
        if key in self.pending:
            copy, cond = self.pending.pop(key)
            self.under(cond, copy.wait_send)

    def drain(self):
        for key in list(self.pending):
            self.settle(key)


def layer_kernel(
    q_hbm,
    k_hbm,
    v_hbm,
    doc_ref,
    res_hbm,
    post_hbm,
    ffn_hbm,
    tables_hbm,
    ow_hbm,
    gate_hbm,
    up_hbm,
    mixed_hbm,
    hidden_hbm,
    q_ref,
    res_ref,
    post_ref,
    ffn_ref,
    tables,
    mixed_ref,
    hidden_ref,
    ow,
    w,
    rawk,
    kk,
    vv,
    qrot,
    num,
    den,
    term,
    rs_r,
    rs_l,
    acc,
    x_buf,
    load_sem,
    out_sem,
    pair_send,
    pair_recv,
    xy_send,
    k_recv,
    v_recv,
    z_send,
    z_recv,
    w_recv,
    far_recv,
):
    dp = lax.axis_index("dp")
    c = lax.axis_index("ctx")
    t = lax.axis_index("tensor")
    row = c // 8
    x = (c % 8) // 2
    core = c % 2
    par = t % 2

    def at(r, xx, kk_, d=dp):
        return (d, r * 8 + xx * 2 + kk_, t)

    x_up = (x + 1) % 4
    x_dn = (x + 3) % 4
    right_x = at(row, x_up, core)
    left_x = at(row, x_dn, core)
    cross = at(1 - row, x, core)
    sib = at(row, x, 1 - core)
    z_up = (dp, c, (t + 1) % RING)
    z_dn = (dp, c, (t + RING - 1) % RING)
    mate = (dp, c, t + 1 - 2 * par)
    twin = at(row, x, core, 1 - dp)
    other = at(1 - row, x, core, 1 - dp)

    barrier = pltpu.get_barrier_semaphore()
    friends = (right_x, left_x, cross, sib, z_up, z_dn, twin, other)
    for friend in friends:
        pl.semaphore_signal(barrier, inc=1, device_id=friend, device_id_type=MESH)
    own_lanes = pl.ds(pl.multiple_of(par * HALF, HALF), HALF)

    def load(i, src, dst):
        copy = pltpu.make_async_copy(src, dst, load_sem.at[i])
        copy.start()
        return copy

    got_k = load(0, k_hbm, rawk.at[par])
    got_v = load(1, v_hbm, vv.at[c, :, own_lanes])
    got_q = load(2, q_hbm, q_ref)
    got_tables = load(3, tables_hbm, tables)
    got_ow = load(4, ow_hbm, ow)
    got_norm = [
        load(5 + i, src, dst)
        for i, (src, dst) in enumerate(((res_hbm, res_ref), (post_hbm, post_ref), (ffn_hbm, ffn_ref)))
    ]
    own_rows = pl.ds(pl.multiple_of(c * SHARD, 16), SHARD)
    for n in range(TILES):
        for i, ref in enumerate((gate_hbm, up_hbm)):
            pltpu.make_async_copy(
                ref.at[:, pl.ds(n * 128, 128)],
                w.at[own_rows, pl.ds(n * 256 + i * 128, 128)],
                load_sem.at[8],
            ).start()

    sends = Sends()

    def remote(src, dst, send, recv, to):
        return pltpu.make_async_remote_copy(
            src_ref=src, dst_ref=dst, send_sem=send, recv_sem=recv, device_id=to, device_id_type=MESH
        )

    def attend(b, n):
        lane = b * TOK + lax.broadcasted_iota(jnp.int32, (1, n * TOK), 1)
        keys = kk[pl.ds(b, n)].reshape(n * TOK, HEAD)
        values = vv[pl.ds(b, n)].reshape(n * TOK, HEAD)
        scores = lax.dot_general(qrot[...], keys, (((1,), (1,)), ((), ())), preferred_element_type=F32)
        capped = jnp.tanh(scores * (1.0 / (SOFT_CAP * HEAD**0.5))) * (SOFT_CAP / np.log(2.0))
        visible = (lane >= begin) & (lane <= qpos)
        weights = jnp.where(visible, jnp.exp2(capped), 0.0).astype(BF16)
        wide = weights.astype(F32)
        den[...] += functools.reduce(
            jnp.add, [wide[:, i * HALF : (i + 1) * HALF] for i in range(n * TOK // HALF)]
        )
        num[...] += jnp.dot(weights, values, preferred_element_type=F32)

    got_k.wait()
    got_v.wait()
    with jax.named_scope("bar"):
        pl.semaphore_wait(barrier, len(friends))
    pair_k = remote(rawk.at[par], rawk.at[par], pair_send.at[0], pair_recv.at[0], mate)
    own_v = vv.at[c, :, own_lanes]
    pair_v = remote(own_v, own_v, pair_send.at[1], pair_recv.at[1], mate)
    sends.go("pair_k", pair_k)
    sends.go("pair_v", pair_v)

    got_tables.wait()
    cb = tables[pl.ds(2 * TOK + c, 1), :]
    sb = tables[pl.ds(2 * TOK + 16 + c, 1), :]
    cosine = tables[:TOK, :] * cb - tables[TOK : 2 * TOK, :] * sb
    sine = tables[TOK : 2 * TOK, :] * cb + tables[:TOK, :] * sb

    def turned(a, b, where):
        a, b = a.astype(F32), b.astype(F32)
        where[:, :HALF] = (a * cosine - b * sine).astype(BF16)
        where[:, HALF:] = (b * cosine + a * sine).astype(BF16)

    got_q.wait()
    turned(q_ref[:, :HALF], q_ref[:, HALF:], qrot)
    num[...] = jnp.zeros_like(num)
    den[...] = jnp.zeros_like(den)

    qpos = c * TOK + lax.broadcasted_iota(jnp.int32, (TOK, 1), 0)
    begin = jnp.zeros((TOK, 1), jnp.int32)
    total = 0
    for e in range(5):
        total = total + doc_ref[e]
        edge = total * BLOCK
        begin = jnp.where(qpos >= edge, jnp.maximum(begin, edge), begin)


    slot = itertools.cycle(range(POOL))

    def kv_go(ref, recv, b, to, cond):
        i = next(slot)
        sends.go(i, remote(ref.at[b], ref.at[b], xy_send.at[i], recv.at[b], to), cond)

    both = ((kk, k_recv), (vv, v_recv))

    def kv_wait(ref, recv, b, cond):
        got = remote(ref.at[b], ref.at[b], xy_send.at[0], recv.at[b], sib)
        pl.when(cond)(got.wait_recv)

    def spread(ref, recv):
        kv_go(ref, recv, c, cross, row == 0)
        kv_go(ref, recv, c, right_x, x < 3)
        kv_go(ref, recv, c, left_x, x == 0)
        kv_go(ref, recv, c, sib, core == 0)

    with jax.named_scope("pairk"):
        pair_k.wait_recv()
    turned(rawk[0], rawk[1], kk.at[c])
    spread(*both[0])
    with jax.named_scope("pairv"):
        pair_v.wait_recv()
    spread(*both[1])

    mid = (x == 1) | (x == 2)
    lower = row == 1
    even = c - core
    clip = lambda b: jnp.clip(b, 0, 15)

    def come(b, here, onward):
        for ref, recv in both:
            kv_wait(ref, recv, b, here)
            for to, cond in onward:
                kv_go(ref, recv, b, to, cond)

    def attend_pair(first, here):
        theirs = first + 1 - core
        for ref, recv in both:
            kv_wait(ref, recv, theirs, here)
        pl.when(here)(lambda: attend(first, 2))

    def right_going(hop):
        onward = ((right_x, mid),) if hop == 1 else ()
        come(clip(c - 2 * hop), x >= hop, onward + ((sib, x >= hop),))

    def left_going(hop):
        here = lower & (x + hop <= 3)
        onward = ((left_x, lower & mid),) if hop == 1 else ()
        come(clip(c - 8 + 2 * hop), here, onward + ((sib, here),))

    def attend_right(hop):
        attend_pair(clip(even - 2 * hop), x >= hop)

    def attend_left(hop):
        attend_pair(clip(even - 8 + 2 * hop), lower & (x + hop <= 3))

    def shard(r, dx, plane=core):
        return r * 8 + ((x + dx) % 4) * 2 + plane

    def cut(b, start, size):
        return w.at[pl.ds(pl.multiple_of(b * SHARD + start, 16), size), :]

    def w_sem(b, kind):
        return far_recv.at[b // 8] if kind == 2 else w_recv.at[b, kind]

    def w_go(b, start, size, kind, to, cond=None):
        ref = cut(b, start, size)
        i = next(slot)
        sends.go(i, remote(ref, ref, xy_send.at[i], w_sem(b, kind), to), cond)

    def w_wait(b, size, kind):
        ref = cut(b, 0, size)
        remote(ref, ref, xy_send.at[0], w_sem(b, kind), sib).wait_recv()

    main_at = REST * dp
    rest_at = MAIN * dp
    twin_main_at = REST * (1 - dp)
    twin_rest_at = MAIN * (1 - dp)

    def w_across(cond):
        b = shard(row, 0)
        w_go(b, twin_main_at, MAIN, 0, other, cond)
        w_go(b, rest_at, REST, 1, other, cond)

    mine = cut(shard(row, 0), 0, SHARD)
    pltpu.make_async_copy(mine, mine, load_sem.at[8]).wait()
    w_across(lower)
    with jax.named_scope("own"):
        pl.when(core == 0)(lambda: attend(c, 1))
        attend_pair(even, core == 1)
    with jax.named_scope("right1"):
        right_going(1)
    with jax.named_scope("cross"):
        come(
            clip(c - 8),
            lower,
            ((left_x, lower & (x > 0)), (right_x, lower & (x == 3)), (sib, lower & (core == 1))),
        )
    with jax.named_scope("attR1"):
        attend_right(1)
    with jax.named_scope("left1"):
        left_going(1)
    with jax.named_scope("right2"):
        right_going(2)
    with jax.named_scope("right3"):
        right_going(3)
    with jax.named_scope("left3"):
        left_going(3)
    with jax.named_scope("attX"):
        attend_pair(clip(even - 8), lower & (core == 0))
        pl.when(lower & (core == 1))(lambda: attend(clip(c - 8), 1))
    with jax.named_scope("attL1"):
        attend_left(1)
    with jax.named_scope("left2"):
        left_going(2)
    with jax.named_scope("att"):
        attend_right(2)
        attend_right(3)
        attend_left(3)
        attend_left(2)

    def w_first():
        b = shard(row, 0)
        w_across(row == 0)
        w_go(b, main_at, MAIN, 0, right_x)
        w_go(b, main_at, MAIN, 0, left_x)
        w_go(b, 0, SHARD, 0, sib)

    def w_cross():
        b = shard(1 - row, 0)
        w_wait(b, MAIN, 0)
        w_go(b, main_at, MAIN, 0, right_x)
        w_go(b, main_at, MAIN, 0, left_x)
        w_go(b, main_at, MAIN, 0, sib)

    def w_cross_rest():
        b = shard(1 - row, 0)
        w_wait(b, REST, 1)
        w_go(b, twin_rest_at, REST, 1, sib)

    def w_next(r):
        for dx, to, start, size, kind in ((-1, right_x, 0, NEAR, 0), (1, left_x, NEAR, FAR, 2)):
            b = shard(r, dx)
            w_wait(b, MAIN, 0)
            w_go(b, main_at + start, size, kind, to)
            w_go(b, rest_at, REST, 1, at((row + r) % 2, x, core, 1 - dp))
            w_go(b, main_at, MAIN, 0, sib)

    def w_far(r):
        b = shard(r, 2)
        w_wait(b, NEAR, 0)
        w_wait(b, FAR, 2)
        w_go(b, rest_at, REST, 1, twin)
        w_go(b, main_at, MAIN, 0, sib)

    def w_rest(r, dx):
        b = shard(r, dx)
        w_wait(b, REST, 1)
        w_go(b, twin_rest_at, REST, 1, sib)

    def w_last():
        for r in (row, 1 - row):
            for dx in (0, -1, 1, 2):
                b = shard(r, dx, 1 - core)
                if dx == 0 and r is row:
                    w_wait(b, SHARD, 0)
                else:
                    w_wait(b, MAIN, 0)
                    w_wait(b, REST, 1)

    events = {
        ("rs", 4): (lambda: w_next(row),),
        ("rs", 5): (w_cross,),
        ("rs", 6): (lambda: w_far(row),),
        ("rs", 7): (w_cross_rest,),
        ("ag", 2): (lambda: w_next(1 - row),),
        ("ag", 4): (lambda: w_far(1 - row),),
        ("ag", 5): (lambda: w_rest(row, -1), lambda: w_rest(row, 1)),
        ("ag", 7): (lambda: w_rest(row, 2), lambda: w_rest(1 - row, -1), lambda: w_rest(1 - row, 1)),
        ("ag", 8): (lambda: w_rest(1 - row, 2),),
    }
    w_first()
    got_ow.wait()
    sums = jnp.sum(den[...], axis=1, keepdims=True)
    attended = (num[...] / sums).astype(BF16)

    def lanes(s):
        return pl.ds(s * SUB, SUB)

    def block(d):
        return pl.ds(pl.multiple_of(lax.rem(t + d + RING, RING) * ROWS, ROWS), ROWS)

    HOPS = RING // 2
    flows = (
        (0, rs_r, z_up, 1, range(SUBS // 2)),
        (1, rs_l, z_dn, -1, range(SUBS // 2, SUBS)),
    )

    def rs_step(k, s):
        for f, buf, to, sign, early in flows:
            begin_at = 1 if s in early else 2
            if k < begin_at:
                continue
            away = sign * (HOPS + 1 - k)
            if k == begin_at:
                src = term.at[block(away), lanes(s)]
            else:
                src = buf.at[k - 2, :, lanes(s)]
                remote(src, src, z_send.at[f, s], z_recv.at[f, k - 2, s], to).wait_recv()
                buf[k - 2, :, lanes(s)] = (
                    buf[k - 2, :, lanes(s)].astype(F32) + term[block(away), lanes(s)].astype(F32)
                ).astype(BF16)
            sends.go(
                ("z", f, s),
                remote(src, buf.at[k - 1, :, lanes(s)], z_send.at[f, s], z_recv.at[f, k - 1, s], to),
            )

    for s in range(SUBS):
        term[:, lanes(s)] = jnp.dot(attended, ow[:, lanes(s)], preferred_element_type=F32).astype(BF16)
        rs_step(1, s)
    for k in range(2, HOPS + 1):
        with jax.named_scope(f"rs{k}"):
            for s in range(SUBS):
                rs_step(k, s)
        with jax.named_scope(f"rsw{k}"):
            for act in events.get(("rs", k), ()):
                act()

    def whole_row(ref):
        return jnp.concatenate([ref[i : i + 1, :] for i in range(WIDTH // 128)], axis=1)

    for one in got_norm:
        one.wait()
    square = jnp.zeros((ROWS, 1), F32)
    for s in range(SUBS):
        for f, buf, to, _, _ in flows:
            src = buf.at[HOPS - 1, :, lanes(s)]
            remote(src, src, z_send.at[f, s], z_recv.at[f, HOPS - 1, s], to).wait_recv()
        part = (
            term[block(0), lanes(s)].astype(F32)
            + rs_r[HOPS - 1, :, lanes(s)].astype(F32)
            + rs_l[HOPS - 1, :, lanes(s)].astype(F32)
        )
        acc[:, lanes(s)] = part
        square += jnp.sum(part * part, axis=1, keepdims=True)
    scale = lax.rsqrt(square / WIDTH + NORM_EPS)
    mixed = (res_ref[...].astype(F32) + acc[...] * scale * whole_row(post_ref)).astype(BF16)
    mixed_ref[...] = mixed
    mixed_out = pltpu.make_async_copy(mixed_ref, mixed_hbm, out_sem.at[1])
    mixed_out.start()
    wide = mixed.astype(F32)
    scale = lax.rsqrt(jnp.sum(wide * wide, axis=1, keepdims=True) / WIDTH + NORM_EPS)
    x_buf[block(0), :] = (wide * scale * whole_row(ffn_ref)).astype(BF16)

    ag_flows = ((0, z_up, -1, range(SUBS // 2)), (1, z_dn, 1, range(SUBS // 2, SUBS)))

    def ag_got(k, s):
        for f, to, sign, late in ag_flows:
            if k == HOPS and s not in late:
                continue
            src = x_buf.at[block(sign * k), lanes(s)]
            remote(src, src, z_send.at[f, s], z_recv.at[f, k - 1, s], to).wait_recv()

    for k in range(1, HOPS + 1):
        with jax.named_scope(f"ag{k}"):
            for s in range(SUBS):
                for f, to, sign, late in ag_flows:
                    if k > 1:
                        got = x_buf.at[block(sign * (k - 1)), lanes(s)]
                        remote(got, got, z_send.at[f, s], z_recv.at[f, k - 2, s], to).wait_recv()
                    if k == HOPS and s not in late:
                        continue
                    src = x_buf.at[block(sign * (k - 1)), lanes(s)]
                    sends.go(("z", f, s), remote(src, src, z_send.at[f, s], z_recv.at[f, k - 1, s], to))
        with jax.named_scope(f"agw{k}"):
            for act in events.get(("ag", k), ()):
                act()
    with jax.named_scope("aglast"):
        for s in range(SUBS):
            ag_got(HOPS, s)
    with jax.named_scope("wlast"):
        w_last()

    with jax.named_scope("ffn"):
        for n in range(TILES):
            both_parts = jnp.dot(x_buf[...], w[:, pl.ds(n * 256, 256)], preferred_element_type=F32)
            gate, up = both_parts[:, :128], both_parts[:, 128:]
            tile = pl.ds(n * 128, 128)
            hidden_ref[:, tile] = (jax.nn.gelu(gate, approximate=True) * up).astype(BF16)
            out = pltpu.make_async_copy(hidden_ref.at[:, tile], hidden_hbm.at[:, tile], out_sem.at[0])
            out.start()
    with jax.named_scope("drain"):
        sends.drain()
        mixed_out.wait()
        pltpu.make_async_copy(hidden_ref, hidden_hbm, out_sem.at[0]).wait()


def layer(q, k, v, doc_blocks, residual, post_gain, ffn_gain, out_weight, gate, up):
    hbm = pl.BlockSpec(memory_space=pl.ANY)
    half = RING // 2
    dma = pltpu.SemaphoreType.DMA
    vmem = pltpu.VMEM
    return pl.pallas_call(
        layer_kernel,
        out_shape=(
            jax.ShapeDtypeStruct((ROWS, WIDTH), BF16),
            jax.ShapeDtypeStruct((TOK, COLS), BF16),
        ),
        in_specs=[hbm] * 3 + [pl.BlockSpec(memory_space=pltpu.SMEM)] + [hbm] * 7,
        out_specs=(hbm, hbm),
        scratch_shapes=[
            vmem((TOK, HEAD), BF16),
            vmem((ROWS, WIDTH), BF16),
            vmem((WIDTH // 128, 128), F32),
            vmem((WIDTH // 128, 128), F32),
            vmem((2 * TOK + 32, HALF), F32),
            vmem((ROWS, WIDTH), BF16),
            vmem((TOK, COLS), BF16),
            vmem((HEAD, WIDTH), BF16),
            vmem((16 * SHARD, 2 * COLS), BF16),
            vmem((2, TOK, HALF), BF16),
            vmem((16, TOK, HEAD), BF16),
            vmem((16, TOK, HEAD), BF16),
            vmem((TOK, HEAD), BF16),
            vmem((TOK, HEAD), F32),
            vmem((TOK, HALF), F32),
            vmem((TOK, WIDTH), BF16),
            vmem((half, ROWS, WIDTH), BF16),
            vmem((half, ROWS, WIDTH), BF16),
            vmem((ROWS, WIDTH), F32),
            vmem((TOK, WIDTH), BF16),
            dma((9,)),
            dma((2,)),
            dma((2,)),
            dma((2,)),
            dma((POOL,)),
            dma((16,)),
            dma((16,)),
            dma((2, SUBS)),
            dma((2, half, SUBS)),
            dma((16, 2)),
            dma((2,)),
        ],
        compiler_params=pltpu.CompilerParams(
            collective_id=0, has_side_effects=True, vmem_limit_bytes=56 * 1024 * 1024
        ),
        cost_estimate=pl.CostEstimate(flops=2_000_000_000, bytes_accessed=8_000_000, transcendentals=0),
    )(
        q,
        k,
        v,
        doc_blocks,
        residual,
        post_gain.reshape(WIDTH // 128, 128),
        ffn_gain.reshape(WIDTH // 128, 128),
        jnp.asarray(rope_tables()),
        out_weight,
        gate,
        up,
    )


def per_device(
    residual,
    queries,
    key_heads,
    value_heads,
    doc_blocks,
    out_weight,
    post_gain,
    ffn_gain,
    gate_weight,
    up_weight,
):
    return layer(
        queries,
        key_heads,
        value_heads,
        doc_blocks,
        residual,
        post_gain,
        ffn_gain,
        out_weight,
        gate_weight,
        up_weight,
    )


def solution(mesh):
    in_specs = (
        P(("dp", "ctx", "tensor"), None),
        P(("dp", "ctx"), "tensor"),
        P(("dp", "ctx"), "tensor"),
        P(("dp", "ctx"), "tensor"),
        P("dp"),
        P("tensor", None),
        P(),
        P(),
        P("ctx", "tensor"),
        P("ctx", "tensor"),
    )
    out_specs = (P(("dp", "ctx", "tensor"), None), P(("dp", "ctx"), "tensor"))
    return jax.shard_map(
        per_device, mesh=mesh, in_specs=in_specs, out_specs=out_specs, check_vma=False
    )
```
